256 devices in a mesh: rep: 2 (over z), blk: 128 (over x, y, core).
Axes of the slice: x: 8, y: 8, z: 2, core: 2. Of those that a mesh axis runs over, the one named last changes fastest.
The devices are a block of a 8x8x16 slice.
Arguments:
- hidden: bfloat16 [32, 4096], P('rep', 'blk'), parts along dimension 0, may hold values from -4 to 4
- queries: bfloat16 [32, 4096], P('rep'), parts along dimension 0, may hold values from -180 to 180
- cache_kv: bfloat16 [2, 32, 4096, 1024], P(None, 'rep', 'blk'), parts along dimension 1, may hold values from -6 to 6
- cache_len: int32 [32], P('rep'), parts along dimension 0, may hold values from 1 to 4096
- inserted_key_value: bfloat16 [2, 16, 4096, 1024], P(None, 'rep', 'blk'), parts along dimension 1, may hold values from -6 to 6
- insert_slot: int32 [16], P('rep'), parts along dimension 0, may hold values from 0 to 15, as said below
- prefix_len: int32 [16], P('rep'), parts along dimension 0, may hold values from 1 to 4096, as said below
- out_weight: bfloat16 [4096, 4096], P(None, 'blk'), may hold values from -0.09375 to 0.09375
- norm_gain: bfloat16 [4096], replicated, may hold values from 0.25 to 1.75
- router_weight: bfloat16 [4096, 4], replicated, may hold values from -0.09375 to 0.09375
- expert_ids: int32 [32, 2], P('rep'), parts along dimension 0, may hold values from 0 to 3, all different within a row
- gate_up: bfloat16 [2, 4096, 28672], P(None, None, 'blk'), may hold values from -0.09375 to 0.09375
- down_proj: bfloat16 [28672, 4096], P('blk'), may hold values from -0.0625 to 0.0625
Outputs:
- layer_out: bfloat16 [32, 4096], P('rep', 'blk'), parts along dimension 0
The draws below stay inside these ranges and needn't reach their ends.
There are 2 independent parts, one for each index of `rep`. The reference program is written for one: setup_inputs(seed, part) draws one part's arguments, and reference() takes and returns one part's arrays. A program takes and returns all parts, laid end to end along the dimension named above; an argument that names none is the same for every part. Nothing has to cross between parts.
Inputs may be any that keep to these rules, and one draw needn't show every extreme that they name: `insert_slot`: 8 different slot numbers. `prefix_len`: some inserted request has all 4096 positions.
All inputs are finite; a program needn't handle non-finite values.
Results may differ from the reference program's by a relative error of at most 0.012.
Values may be sent and summed in bfloat16 or wider, within the bound.
A program may use at most 128 MiB of HBM per device.

```python
import math
import jax
import jax.numpy as jnp
from jax import lax

D = 4096
QUERY_HEADS = 32
KEY_VALUE_HEADS = 8
HEAD_SIZE = 128
EXPERTS = 4
FF = 7168
SLOTS = 16
INSERTED_SLOTS = 8
CACHE_POSITIONS = 4096


def slot_order(key):
    return jax.random.permutation(jax.random.fold_in(key, 11), SLOTS).astype(jnp.int32)


def cache_lengths(key):
    return jax.random.randint(jax.random.fold_in(key, 12), (SLOTS,), 1, CACHE_POSITIONS + 1).astype(jnp.int32)


def rows_per_slot(key, slot_entry):
    cache_rows = jax.random.normal(jax.random.fold_in(jax.random.fold_in(key, 13), slot_entry), (2, CACHE_POSITIONS, KEY_VALUE_HEADS * HEAD_SIZE), jnp.float32)
    return jnp.clip(cache_rows, -6.0, 6.0)


def inserted_rows(key):
    drawn = jax.random.normal(jax.random.fold_in(key, 41), (2, INSERTED_SLOTS, CACHE_POSITIONS, KEY_VALUE_HEADS * HEAD_SIZE), jnp.float32)
    return jnp.clip(drawn, -6.0, 6.0)


def longest_request(key):
    return jax.random.randint(jax.random.fold_in(key, 32), (), 0, INSERTED_SLOTS).astype(jnp.int32)


def draw_insert_slot(key, part):
    return slot_order(key)[:INSERTED_SLOTS]


def draw_prefix_len(key, part):
    drawn = jax.random.randint(jax.random.fold_in(key, 31), (INSERTED_SLOTS,), 1, CACHE_POSITIONS + 1).astype(jnp.int32)
    longest = longest_request(key)
    return jnp.where(jnp.arange(INSERTED_SLOTS, dtype=jnp.int32) == longest, CACHE_POSITIONS, drawn).astype(jnp.int32)


def draw_cache_len(key, part):
    return cache_lengths(key)


def draw_inserted_key_value(key, part):
    return inserted_rows(key).astype(jnp.bfloat16)


def draw_cache_kv(key, part):
    every_entry = jax.vmap(lambda slot_entry: rows_per_slot(key, slot_entry))(jnp.arange(SLOTS, dtype=jnp.int32))
    return jnp.transpose(every_entry, (1, 0, 2, 3)).astype(jnp.bfloat16)


def draw_queries(key, part):
    base = jnp.clip(1.5 * jax.random.normal(jax.random.fold_in(key, 21), (SLOTS, QUERY_HEADS * HEAD_SIZE), jnp.float32), -9.0, 9.0)
    longest = longest_request(key)
    target_slot = slot_order(key)[longest]
    final_keys = inserted_rows(key)[0, longest, CACHE_POSITIONS // 2 - 1].astype(jnp.bfloat16).astype(jnp.float32).reshape(KEY_VALUE_HEADS, 1, HEAD_SIZE)
    final_query = jnp.broadcast_to(4.0 * final_keys, (KEY_VALUE_HEADS, QUERY_HEADS // KEY_VALUE_HEADS, HEAD_SIZE)).reshape(QUERY_HEADS * HEAD_SIZE)
    base = base.at[target_slot].set(final_query)
    return base.astype(jnp.bfloat16)


def levels(stream_key, extent, cuts, low, largest):
    def one(axis_at, shards_of):
        draws = jax.random.uniform(jax.random.fold_in(jax.random.fold_in(stream_key, 6), axis_at), (shards_of,), jnp.float32, low / len(cuts), largest / len(cuts))
        return jnp.repeat(jnp.exp(draws), extent[axis_at] // shards_of).reshape((-1,) + (1,) * (len(extent) - axis_at - 1))

    level = one(*cuts[0])
    for cut in cuts[1:]:
        level = level * one(*cut)
    return level


def choose_distinct(stream_key, rows, count, top, lift):
    sequence = jax.random.permutation(jax.random.fold_in(stream_key, 1), count)
    boost = sequence
    for power in range(3):
        boost = boost * boost // count
    boost = boost * lift // count
    tickets = jax.random.randint(jax.random.fold_in(stream_key, 2), (rows, count), 0, 4096) + boost
    sure = jax.random.permutation(jax.random.fold_in(stream_key, 3), rows)[jnp.arange(count) % rows]
    tickets = jnp.where(jnp.arange(rows)[:, None] == sure[None, :], 1 << 14, tickets)
    priority = tickets * count + jnp.arange(count)
    return lax.top_k(priority.astype(jnp.int32), top)[1].astype(jnp.int32)


def bell_draw(stream_key, shape, deviation, reach, split=(), held_as=jnp.bfloat16):
    factor_of = levels(stream_key, shape, split, -0.22, 0.18) if split else 1.0
    result = jax.random.normal(stream_key, shape, jnp.float32) * deviation * factor_of
    return jnp.minimum(jnp.maximum(result, -reach), reach).astype(held_as)


def setup_inputs(seed: int = 0, part: int = 0) -> dict:
    splits = jax.random.split(jax.random.key(seed), 14)
    part_splits = jax.random.split(jax.random.fold_in(splits[13], part), 14)
    return {
        "hidden": bell_draw(part_splits[0], (SLOTS, D), 0.3, 4.0, ((1, 128),)),
        "queries": draw_queries(jax.random.fold_in(jax.random.fold_in(splits[13], part), 71), part),
        "cache_kv": draw_cache_kv(jax.random.fold_in(jax.random.fold_in(splits[13], part), 71), part),
        "cache_len": draw_cache_len(jax.random.fold_in(jax.random.fold_in(splits[13], part), 71), part),
        "inserted_key_value": draw_inserted_key_value(jax.random.fold_in(jax.random.fold_in(splits[13], part), 71), part),
        "insert_slot": draw_insert_slot(jax.random.fold_in(jax.random.fold_in(splits[13], part), 71), part),
        "prefix_len": draw_prefix_len(jax.random.fold_in(jax.random.fold_in(splits[13], part), 71), part),
        "out_weight": bell_draw(splits[7], (QUERY_HEADS * HEAD_SIZE, D), (QUERY_HEADS * HEAD_SIZE) ** -0.5, 0.09375, ((1, 128),)),
        "norm_gain": jnp.clip(1.0 + 0.15 * jax.random.normal(splits[8], (D,), jnp.float32), 0.25, 1.75).astype(jnp.bfloat16),
        "router_weight": bell_draw(splits[9], (D, EXPERTS), D ** -0.5, 0.09375),
        "expert_ids": choose_distinct(part_splits[10], SLOTS, EXPERTS, 2, 8192),
        "gate_up": bell_draw(splits[11], (2, D, EXPERTS * FF), D ** -0.5, 0.09375, ((2, 128),)),
        "down_proj": bell_draw(splits[12], (EXPERTS * FF, D), FF ** -0.5, 0.0625, ((0, 128),)),
    }


def attend(queries, key_rows, value_rows, slot_lengths):
    slot_list = queries.shape[0]
    query_groups = QUERY_HEADS // KEY_VALUE_HEADS
    heads_of_queries = queries.astype(jnp.float32).reshape(slot_list, KEY_VALUE_HEADS, query_groups, HEAD_SIZE)
    heads_of_keys = key_rows.astype(jnp.float32).reshape(slot_list, -1, KEY_VALUE_HEADS, HEAD_SIZE)
    heads_of_values = value_rows.astype(jnp.float32).reshape(slot_list, -1, KEY_VALUE_HEADS, HEAD_SIZE)
    scores = jnp.einsum('skgd,sckd->skgc', heads_of_queries, heads_of_keys) / math.sqrt(HEAD_SIZE)
    positions = jnp.arange(heads_of_keys.shape[1], dtype=jnp.int32)
    masked = (positions[None, :] < slot_lengths[:, None])[:, None, None, :]
    scores = jnp.where(masked, scores, -1e+30)
    peak = lax.optimization_barrier(jnp.max(scores, axis=-1, keepdims=True))
    weights = jnp.where(masked, jnp.exp(scores - peak), 0.0)
    totals = lax.optimization_barrier(jnp.sum(weights, axis=-1))
    mixed_values = jnp.einsum('skgc,sckd->skgd', weights, heads_of_values)
    return (mixed_values / totals[..., None]).reshape(slot_list, QUERY_HEADS * HEAD_SIZE)

def route_shares(normed, router_weight, expert_ids):
    logits = jnp.dot(normed, router_weight, preferred_element_type=jnp.float32)
    chosen = (expert_ids[:, :, None] == jnp.arange(EXPERTS, dtype=jnp.int32)[None, None, :]).astype(jnp.float32)
    picked = lax.optimization_barrier(jnp.sum(chosen * logits[:, None, :], axis=-1))
    gates = jax.nn.sigmoid(picked - picked[:, ::-1])
    return lax.optimization_barrier(jnp.sum(gates[:, :, None] * chosen, axis=1))

def reference(hidden, queries, cache_kv, cache_len, inserted_key_value, insert_slot, prefix_len, out_weight, norm_gain, router_weight, expert_ids, gate_up, down_proj):
    placed = jnp.roll(inserted_key_value, CACHE_POSITIONS // 2, axis=2)
    cache = cache_kv.at[:, insert_slot].set(placed)
    slot_lengths = cache_len.at[insert_slot].set(prefix_len)
    attn = attend(queries, cache[0], cache[1], slot_lengths).astype(jnp.bfloat16)
    mixed = (hidden.astype(jnp.float32) + jnp.dot(attn, out_weight, preferred_element_type=jnp.float32)).astype(jnp.bfloat16)
    mixed_f = mixed.astype(jnp.float32)
    scale = jax.lax.rsqrt(lax.optimization_barrier(jnp.mean(mixed_f * mixed_f, axis=-1, keepdims=True)) + 1e-05)
    normed = (mixed_f * scale * norm_gain.astype(jnp.float32)).astype(jnp.bfloat16)
    shares = route_shares(normed, router_weight, expert_ids)
    moe = jnp.zeros(mixed_f.shape, jnp.float32)
    for expert in range(EXPERTS):
        gate_part = gate_up[0][:, expert * FF:(expert + 1) * FF]
        up_part = gate_up[1][:, expert * FF:(expert + 1) * FF]
        act = (jax.nn.silu(jnp.dot(normed, gate_part, preferred_element_type=jnp.float32)) * jnp.dot(normed, up_part, preferred_element_type=jnp.float32)).astype(jnp.bfloat16)
        moe = moe + shares[:, expert:expert + 1] * jnp.dot(act, down_proj[expert * FF:(expert + 1) * FF], preferred_element_type=jnp.float32)
    return (mixed_f + moe).astype(jnp.bfloat16)
```

```python
import functools
import math

import jax
import jax.numpy as jnp
from jax import lax
from jax.experimental import pallas as pl
from jax.experimental.pallas import tpu as pltpu
from jax.sharding import PartitionSpec as P

QUERY_HEADS = 32
KEY_VALUE_HEADS = 8
HEAD_SIZE = 128
EXPERTS = 4
FF = 7168
GROUP = QUERY_HEADS // KEY_VALUE_HEADS
SIDE = 8
CORES = 2
LANES = 128
PACK = 4
F32 = jnp.float32
BF16 = jnp.bfloat16
MESH = pl.DeviceIdType.MESH
OUT_TYPE = jnp.float32
NT = (((1,), (1,)), ((), ()))


def far_first(t):
    return SIDE // 2 + ((t + 1) // 2) * (1 - 2 * (t % 2))


OFFSETS = [far_first(t) for t in range(SIDE)]
CHIP_OFFSETS = sorted(
    ((dx, dy) for dx in range(SIDE) for dy in range(SIDE)),
    key=lambda o: -(min(o[0], SIDE - o[0]) + min(o[1], SIDE - o[1])),
)


def swap_blocks(top, bottom):
    lane = lax.broadcasted_iota(jnp.int32, top.shape, 2)
    sub = lax.broadcasted_iota(jnp.int32, top.shape, 1)
    low = lane < 64
    odd = (lane // 32) % 2 == 1
    keep = (sub >= 4) == odd

    def inner(x):
        y = pltpu.roll(x, 4, 1)
        return jnp.where(keep, x, jnp.where(odd, pltpu.roll(y, 32, 2), pltpu.roll(y, 96, 2)))

    new_top = jnp.where(low, top, pltpu.roll(bottom, 64, 2))
    new_bottom = jnp.where(low, pltpu.roll(top, 64, 2), bottom)
    return inner(new_top), inner(new_bottom)


def layer(
    cache_len_h,
    insert_slot_h,
    prefix_len_h,
    expert_ids_h,
    hidden,
    queries,
    cache_kv,
    inserted_kv,
    out_weight,
    gain,
    router,
    gate_up,
    down,
    out,
    cache_len,
    insert_slot,
    prefix_len,
    expert_ids,
    hidden_v,
    q_v,
    kv_v,
    wo_v,
    gain_v,
    gain_rows,
    router_v,
    gu_v,
    down_v,
    part_send,
    part_recv,
    attn_send,
    attn_v,
    mix_send,
    mix_v,
    moe_send,
    moe_recv,
    load_sem,
    send_sem,
    recv_sem,
):
    me = lax.axis_index("blk")
    n = lax.axis_size("blk")
    chip, core = me // CORES, me % CORES
    x, y = chip // SIDE, chip % SIDE
    is_owner = core == CORES - 1
    slots = hidden.shape[0]
    width = hidden.shape[1]
    inserts = inserted_kv.shape[1]
    rows = cache_kv.shape[2]
    positions = rows * n
    entries = slots + inserts
    owners = n // CORES
    column_devices = n // SIDE
    column_tiles = column_devices // PACK
    column_width = column_tiles * LANES

    def device(cx, cy, cc):
        return {"blk": (cx * SIDE + cy) * CORES + cc}

    def to_all():
        for dx, dy in CHIP_OFFSETS:
            for dc in range(CORES):
                if (dx, dy, dc) != (0, 0, 0):
                    yield OFFSETS.index(dx), device(
                        (x + dx) % SIDE, (y + dy) % SIDE, (core + dc) % CORES
                    )

    def column_from(t):
        return (x + SIDE - OFFSETS[t]) % SIDE

    barrier = pltpu.get_barrier_semaphore()

    @pl.when(is_owner)
    def _():
        for _, peer in to_all():
            pl.semaphore_signal(barrier, inc=1, device_id=peer, device_id_type=MESH)

    loads = iter(range(load_sem.shape[0]))

    def load(pairs):
        k = next(loads)
        for src, dst in pairs:
            pltpu.make_async_copy(src, dst, load_sem.at[k]).start()
        return k

    def loaded(dst, k):
        pltpu.make_async_copy(dst, dst, load_sem.at[k]).wait()

    small = [
        (dst, load([(src, dst)]))
        for src, dst in (
            (cache_len_h, cache_len),
            (insert_slot_h, insert_slot),
            (prefix_len_h, prefix_len),
        )
    ]
    column_kv = []
    column_q = []
    for t in range(SIDE):
        g = (x + OFFSETS[t]) % SIDE
        q_cols = pl.ds(pl.multiple_of(g * GROUP * LANES, LANES), GROUP * LANES)
        head = pl.ds(pl.multiple_of(g * LANES, LANES), LANES)
        column_q.append(load([(queries.at[:, q_cols], q_v.at[t])]))
        pairs = []
        for part in range(2):
            pairs.append((cache_kv.at[part, :, :, head], kv_v.at[t, part, pl.ds(0, slots)]))
            pairs.append(
                (inserted_kv.at[part, :, :, head], kv_v.at[t, part, pl.ds(slots, inserts)])
            )
        column_kv.append(load(pairs))
    hidden_k = load([(hidden, hidden_v)])
    ids_k = load([(expert_ids_h, expert_ids)])

    for dst, k in small:
        loaded(dst, k)
    column = lax.broadcasted_iota(jnp.int32, (1, entries * rows), 1)
    entry, at = column // rows, me * rows + column % rows
    at = jnp.where(entry < slots, at, (at + positions // 2) % positions)
    owner_slot = jnp.where(entry < slots, entry, -1)
    limit = jnp.zeros_like(column)
    for s in range(slots):
        limit = jnp.where(entry == s, cache_len[s], limit)
    for j in range(inserts):
        owner_slot = jnp.where(entry == insert_slot[j], -1, owner_slot)
    for j in range(inserts):
        owner_slot = jnp.where(entry == slots + j, insert_slot[j], owner_slot)
        limit = jnp.where(entry == slots + j, prefix_len[j], limit)
    owner_slot = jnp.where(at < limit, owner_slot, -1)
    row_slot = lax.broadcasted_iota(jnp.int32, (GROUP * slots, 1), 0) % slots
    mask = row_slot == owner_slot
    stat_lane = lax.broadcasted_iota(jnp.int32, (GROUP * slots, LANES), 1)
    half_lane = lax.broadcasted_iota(jnp.int32, (SIDE, 4, LANES), 2) < 64

    def score(t):
        loaded(q_v.at[t], column_q[t])
        loaded(kv_v.at[t], column_kv[t])
        q = jnp.concatenate([q_v[t, :, i * LANES : (i + 1) * LANES] for i in range(GROUP)], axis=0)
        keys = kv_v[t, 0].reshape(entries * rows, LANES)
        return lax.dot_general(q, keys, NT, preferred_element_type=F32) * (
            1.0 / math.sqrt(HEAD_SIZE)
        )

    scores = score(0)
    for t in range(SIDE):
        following = score(t + 1) if t + 1 < SIDE else None
        scores = jnp.where(mask, scores, -1e30)
        peak = jnp.max(scores, axis=1, keepdims=True).astype(BF16).astype(F32)
        weights = jnp.where(mask, jnp.exp(scores - peak), 0.0).astype(BF16)
        total = jnp.sum(weights.astype(F32), axis=1, keepdims=True)
        values = kv_v[t, 1].reshape(entries * rows, LANES)
        mixed_values = jnp.dot(weights, values, preferred_element_type=F32)
        rounded = total.astype(BF16).astype(F32)
        mixed_values = mixed_values * (rounded / jnp.maximum(total, 1e-30))
        stats = jnp.where((stat_lane // 32) % 2 == 0, peak, rounded).reshape(SIDE, 8, LANES)
        stats = jnp.where(half_lane, stats[:, 0:4], stats[:, 4:8])
        g = (x + OFFSETS[t]) % SIDE
        part_send[t, :, 0:8, :] = mixed_values.reshape(SIDE, 8, LANES).astype(BF16)
        part_send[t, :, 8:12, :] = stats.astype(BF16)
        if t == 0:

            @pl.when(is_owner)
            def _():
                pl.semaphore_wait(barrier, owners - 1)

            @pl.when(core != CORES - 1)
            def _():
                pl.semaphore_wait(barrier, owners)

        for dy in OFFSETS:
            cy = (y + dy) % SIDE
            copy = functools.partial(
                pltpu.make_async_remote_copy,
                src_ref=part_send.at[t, cy],
                dst_ref=part_recv.at[me],
                send_sem=send_sem.at[0],
                recv_sem=recv_sem.at[0, t],
                device_id=device(g, cy, CORES - 1),
                device_id_type=MESH,
            )
            if OFFSETS[t] == 0 and dy == 0:

                @pl.when(is_owner)
                def _():
                    pltpu.make_async_copy(
                        part_send.at[t, cy], part_recv.at[me], recv_sem.at[0, t]
                    ).start()

                @pl.when(core != CORES - 1)
                def _():
                    copy().start()
            else:
                copy().start()
        scores = following

    wo_k = load(
        [(out_weight, wo_v.at[pl.ds(k * width, width)]) for k in range(PACK)]
    )
    gain_k = load([(gain, gain_v)])
    router_k = load([(router, router_v)])
    gu_k = load([(gate_up.at[part], gu_v.at[part]) for part in range(2)])
    down_k = load([(down, down_v)])

    half_rows = slots // 2

    @pl.when(is_owner)
    def _():
        lane8 = lax.broadcasted_iota(jnp.int32, (1, 8, LANES), 2)
        lower = lax.broadcasted_iota(jnp.int32, (1, 8, LANES), 1) < 4

        def spread(v):
            v = jnp.where(lane8 < 32, v, pltpu.roll(v, 32, 2))
            return jnp.where(lane8 < 64, v, pltpu.roll(v, 64, 2))

        best = jnp.full((1, 8, LANES), -3e38, F32)
        sums = jnp.zeros((1, 8, LANES), F32)
        totals = jnp.zeros((1, 8, LANES), F32)
        for t in reversed(range(SIDE)):
            here = part_recv.at[pl.ds(column_from(t) * column_devices, column_devices)]
            pltpu.make_async_copy(here, here, recv_sem.at[0, t]).wait()
            got = here[...].astype(F32)
            s = jnp.concatenate([got[:, 8:12], got[:, 8:12]], axis=1)
            s = jnp.where(lower, s, pltpu.roll(s, 64, 2))
            high = spread(jnp.maximum(best, jnp.max(s, axis=0, keepdims=True)))
            old = jnp.exp(best - high)
            e = spread(jnp.exp(jnp.where(lane8 < 32, s - high, 0.0)))
            sums = sums * old + jnp.sum(got[:, 0:8] * e, axis=0, keepdims=True)
            totals = totals * old + jnp.sum(s * e, axis=0, keepdims=True)
            best = high
        totals = spread(pltpu.roll(totals, 96, 2))
        attn_send[...] = (sums / totals)[0].astype(BF16)
        mine = attn_v.at[
            chip // 2, pl.ds(pl.multiple_of((chip % 2) * half_rows, half_rows), half_rows)
        ]
        pltpu.make_async_copy(attn_send, mine, recv_sem.at[1, OFFSETS.index(0)]).start()
        for t, peer in to_all():
            pltpu.make_async_remote_copy(
                src_ref=attn_send,
                dst_ref=mine,
                send_sem=send_sem.at[1],
                recv_sem=recv_sem.at[1, t],
                device_id=peer,
                device_id_type=MESH,
            ).start()

    loaded(expert_ids, ids_k)
    slot_row = lax.broadcasted_iota(jnp.int32, (slots, 1), 0)
    first = jnp.zeros((slots, 1), jnp.int32)
    second = jnp.zeros((slots, 1), jnp.int32)
    for s in range(slots):
        first = jnp.where(slot_row == s, expert_ids[0, s], first)
        second = jnp.where(slot_row == s, expert_ids[1, s], second)
    loaded(hidden_v, hidden_k)
    mixed_4 = jnp.concatenate([hidden_v[...].astype(F32)] * PACK, axis=1)
    loaded(gain_v, gain_k)
    for i in range(gain_v.shape[0]):
        gain_rows[i] = jnp.broadcast_to(gain_v[i : i + 1, :].astype(F32), (8, LANES))

    loaded(wo_v, wo_k)
    for t in reversed(range(SIDE)):
        cx = column_from(t)
        here = attn_v.at[pl.ds(cx * GROUP, GROUP)]
        pltpu.make_async_copy(here, here, recv_sem.at[1, t]).wait()
        attn = jnp.concatenate([here[i] for i in range(GROUP)], axis=1)
        cols = pl.ds(pl.multiple_of(cx * GROUP * LANES, LANES), GROUP * LANES)
        mixed_4 = mixed_4 + lax.dot_general(attn, wo_v[:, cols], NT, preferred_element_type=F32)
    mixed_4 = mixed_4.astype(BF16).astype(F32)
    block = lax.broadcasted_iota(jnp.int32, (PACK, LANES), 1) // width
    packed = jnp.zeros((PACK, LANES), F32)
    for k in range(PACK):
        packed = jnp.where(block == k, mixed_4[k * PACK : (k + 1) * PACK], packed)
    mix_send[...] = packed.astype(BF16)
    pltpu.make_async_copy(mix_send, mix_v.at[me], recv_sem.at[2, OFFSETS.index(0)]).start()
    for t, peer in to_all():
        pltpu.make_async_remote_copy(
            src_ref=mix_send,
            dst_ref=mix_v.at[me],
            send_sem=send_sem.at[2],
            recv_sem=recv_sem.at[2, t],
            device_id=peer,
            device_id_type=MESH,
        ).start()

    loaded(router_v, router_k)
    loaded(gu_v, gu_k)
    units = gate_up.shape[1]
    squares = jnp.zeros((slots, LANES), F32)
    gate = jnp.zeros((slots, units), F32)
    up = jnp.zeros((slots, units), F32)
    logits = jnp.zeros((slots, EXPERTS), F32)
    for t in reversed(range(SIDE)):
        cx = column_from(t)
        here = mix_v.at[pl.ds(cx * column_devices, column_devices)]
        pltpu.make_async_copy(here, here, recv_sem.at[2, t]).wait()
        z = here[...].reshape(column_tiles, slots, LANES).astype(F32)
        top, bottom = swap_blocks(z[:, 0:8], z[:, 8:16])
        squares = squares + jnp.concatenate(
            [jnp.sum(top * top, axis=0), jnp.sum(bottom * bottom, axis=0)], axis=0
        )
        gains = gain_rows[pl.ds(cx * column_tiles, column_tiles)]
        z = jnp.concatenate([top * gains, bottom * gains], axis=1).astype(BF16)
        z = jnp.concatenate([z[i] for i in range(column_tiles)], axis=1)
        cols = pl.ds(pl.multiple_of(cx * column_width, LANES), column_width)
        gate = gate + lax.dot_general(z, gu_v[0, :, cols], NT, preferred_element_type=F32)
        up = up + lax.dot_general(z, gu_v[1, :, cols], NT, preferred_element_type=F32)
        logits = logits + lax.dot_general(z, router_v[:, cols], NT, preferred_element_type=F32)
    mean = jnp.sum(squares, axis=1, keepdims=True) / (n * width)
    scale = lax.rsqrt(mean + 1e-05)
    gate = gate * scale
    act = (gate * jax.nn.sigmoid(gate) * (up * scale)).astype(BF16)

    logits = logits * scale
    expert = lax.broadcasted_iota(jnp.int32, (slots, EXPERTS), 1)
    logit_a = jnp.sum(jnp.where(expert == first, logits, 0.0), axis=1, keepdims=True)
    logit_b = jnp.sum(jnp.where(expert == second, logits, 0.0), axis=1, keepdims=True)
    expert_now = me * units // FF
    share = jnp.where(first == expert_now, jax.nn.sigmoid(logit_a - logit_b), 0.0) + jnp.where(
        second == expert_now, jax.nn.sigmoid(logit_b - logit_a), 0.0
    )

    loaded(down_v, down_k)

    def product(t):
        cx = (x + OFFSETS[t]) % SIDE
        cols = pl.ds(pl.multiple_of(cx * column_width, LANES), column_width)
        return jnp.dot(act, down_v[:, cols], preferred_element_type=F32)

    term = product(0)
    for t in range(SIDE):
        following = product(t + 1) if t + 1 < SIDE else None
        cx = (x + OFFSETS[t]) % SIDE
        term = term * share
        term = jnp.stack([term[:, i * LANES : (i + 1) * LANES] for i in range(column_tiles)], axis=0)
        top, bottom = swap_blocks(term[:, 0:8], term[:, 8:16])
        both = jnp.concatenate([top, bottom], axis=1).astype(BF16)
        moe_send[t] = both.reshape(column_devices, PACK, LANES)
        for dy in OFFSETS:
            for dc in range(CORES):
                cy, cc = (y + dy) % SIDE, (core + dc) % CORES
                source = moe_send.at[t, cy * CORES + cc]
                if (OFFSETS[t], dy, dc) == (0, 0, 0):
                    pltpu.make_async_copy(source, moe_recv.at[me], recv_sem.at[3, t]).start()
                else:
                    pltpu.make_async_remote_copy(
                        src_ref=source,
                        dst_ref=moe_recv.at[me],
                        send_sem=send_sem.at[3],
                        recv_sem=recv_sem.at[3, t],
                        device_id=device(cx, cy, cc),
                        device_id_type=MESH,
                    ).start()
        term = following

    @pl.when(is_owner)
    def _():
        sent = part_recv.at[pl.ds(0, owners - 1)]
        pltpu.make_async_copy(sent, sent, send_sem.at[0]).wait()
        sent = part_recv.at[pl.ds(0, n - 1), pl.ds(0, half_rows)]
        pltpu.make_async_copy(sent, sent, send_sem.at[1]).wait()

    @pl.when(core != CORES - 1)
    def _():
        pltpu.make_async_copy(part_send, part_send, send_sem.at[0]).wait()

    sent = mix_v.at[pl.ds(0, n - 1)]
    pltpu.make_async_copy(sent, sent, send_sem.at[2]).wait()

    final = packed
    moe = jnp.zeros((slots, LANES), F32)
    for t in reversed(range(SIDE)):
        here = moe_recv.at[pl.ds(column_from(t) * column_devices, column_devices)]
        pltpu.make_async_copy(here, here, recv_sem.at[3, t]).wait()
        z = here[...].reshape(column_tiles, slots, LANES).astype(F32)
        moe = moe + jnp.sum(z, axis=0)
    for k in range(PACK):
        final = final + moe[k * PACK : (k + 1) * PACK]
    out[...] = jnp.concatenate(
        [final[:, k * width : (k + 1) * width] for k in range(PACK)], axis=0
    ).astype(out.dtype)
    sent = mix_v.at[pl.ds(0, n - 1)]
    pltpu.make_async_copy(sent, sent, send_sem.at[3]).wait()


def on_device(
    hidden,
    queries,
    cache_kv,
    cache_len,
    inserted_key_value,
    insert_slot,
    prefix_len,
    out_weight,
    norm_gain,
    router_weight,
    expert_ids,
    gate_up,
    down_proj,
):
    n = lax.axis_size("blk")
    slots, width = hidden.shape
    features = out_weight.shape[0]
    units = gate_up.shape[2]
    rows = cache_kv.shape[2]
    inserts = inserted_key_value.shape[1]
    vmem = pl.BlockSpec(memory_space=pltpu.VMEM)
    hbm = pl.BlockSpec(memory_space=pl.ANY)
    vm, sm = pltpu.VMEM, pltpu.SMEM
    column = n // SIDE
    out = pl.pallas_call(
        layer,
        out_shape=jax.ShapeDtypeStruct(hidden.shape, OUT_TYPE),
        in_specs=[hbm] * 13,
        out_specs=vmem,
        scratch_shapes=[
            sm((slots,), jnp.int32),
            sm((inserts,), jnp.int32),
            sm((inserts,), jnp.int32),
            sm((2, slots), jnp.int32),
            vm((slots, width), BF16),
            vm((SIDE, slots, GROUP * LANES), BF16),
            vm((SIDE, 2, slots + inserts, rows, LANES), BF16),
            vm((PACK * width, features), BF16),
            vm((features // LANES, LANES), BF16),
            vm((features // LANES, 8, LANES), F32),
            vm((EXPERTS, features), BF16),
            vm((2, units, features), BF16),
            vm((units, features), BF16),
            vm((SIDE, SIDE, 12, LANES), BF16),
            vm((n, 12, LANES), BF16),
            vm((slots // 2, LANES), BF16),
            vm((QUERY_HEADS, slots, LANES), BF16),
            vm((PACK, LANES), BF16),
            vm((n, PACK, LANES), BF16),
            vm((SIDE, column, PACK, LANES), BF16),
            vm((n, PACK, LANES), BF16),
            pltpu.SemaphoreType.DMA((26,)),
            pltpu.SemaphoreType.DMA((4,)),
            pltpu.SemaphoreType.DMA((4, SIDE)),
        ],
        compiler_params=pltpu.CompilerParams(collective_id=0, has_side_effects=True),
    )(
        cache_len,
        insert_slot,
        prefix_len,
        expert_ids.T,
        hidden,
        queries,
        cache_kv,
        inserted_key_value,
        out_weight.T,
        norm_gain.reshape(-1, LANES),
        router_weight.T,
        jnp.swapaxes(gate_up, 1, 2),
        down_proj,
    )
    return out.astype(hidden.dtype)


def solution(mesh):
    return jax.shard_map(
        on_device,
        mesh=mesh,
        in_specs=(
            P("rep", "blk"),
            P("rep", None),
            P(None, "rep", "blk", None),
            P("rep"),
            P(None, "rep", "blk", None),
            P("rep"),
            P("rep"),
            P(None, "blk"),
            P(),
            P(),
            P("rep", None),
            P(None, None, "blk"),
            P("blk", None),
        ),
        out_specs=P("rep", "blk"),
        check_vma=False,
    )
```
